32 devices in a mesh: groups: 2 (over x), rows: 8 (over z, y), cols: 2 (over core).
Axes of the slice: x: 2, y: 2, z: 4, core: 2. Of those that a mesh axis runs over, the one named last changes fastest.
Arguments:
- feature_table: float32 [32768, 1024], P(('groups', 'rows'), 'cols'), parts along dimension 0, may hold values from -6 to 6
- own_features: float32 [512, 1024], P(('groups', 'rows'), 'cols'), parts along dimension 0, may hold values from -6 to 6
- neighbor_ids: int32 [512, 50], P(('groups', 'rows')), parts along dimension 0, may hold values from 0 to 16383, as said below
- importance: float32 [512, 50], P(('groups', 'rows')), parts along dimension 0, may hold values from 0.5 to 5
- w_self: bfloat16 [1024, 1024], P('cols'), may hold values from -0.1875 to 0.1875
- w_pool: bfloat16 [1024, 1024], P('cols'), may hold values from -0.1875 to 0.1875
- bias: float32 [1024], replicated, may hold values from -6 to 6
Outputs:
- embeddings: float32 [512, 1024], P(('groups', 'rows'), 'cols'), parts along dimension 0
The draws below stay inside these ranges and needn't reach their ends.
There are 2 independent parts, one for each index of `groups`. The reference program is written for one: setup_inputs(seed, part) draws one part's arguments, and reference() takes and returns one part's arrays. A program takes and returns all parts, laid end to end along the dimension named above; an argument that names none is the same for every part. Nothing has to cross between parts.
Inputs may be any that keep to these rules, and one draw needn't show every extreme that they name: `neighbor_ids`: ids of sampled neighbors in the group's table, repeats allowed. In each aligned block of 16 targets, at most 160 ids fall in any one range [k * 2048, (k + 1) * 2048), and one such range holds exactly 160.
All inputs are finite; a program needn't handle non-finite values.
Results may differ from the reference program's by a relative error of at most 0.0017.
Values may be sent and summed in bfloat16 or wider, within the bound.
A program may use at most 64 MiB of HBM per device.

```python
import math
import jax
import jax.numpy as jnp
from jax import lax

D = 1024
NEIGH = 50
TGT_DEV = 16
ROWS_DEV = 2048
CAP = 160
TARGETS = 256
NODES = 16384


def draw_device(key_device):
    owners = NODES // ROWS_DEV
    per_device = TARGETS // (TGT_DEV * owners)
    slot_count = owners * CAP
    requests = TGT_DEV * NEIGH
    key_busy, key_owner, key_blocks = jax.random.split(key_device, 3)
    slot_index = jnp.arange(slot_count, dtype=jnp.int32)
    labels = slot_index // CAP
    within = slot_index - labels * CAP
    busiest = jax.random.randint(key_busy, (), 0, owners, dtype=jnp.int32)
    owner_order = jax.random.permutation(key_owner, owners).astype(jnp.int32)
    owner_rank = jnp.argsort(owner_order, stable=True).astype(jnp.int32)
    category = jnp.where(labels == busiest, 0, jnp.where(within < CAP - 1, 1, 2)).astype(jnp.int32)
    scores = category * slot_count + owner_rank[labels] * CAP + within
    ordering = jnp.argsort(scores, stable=True)
    chosen = labels[ordering[:requests]]
    block_keys = jax.random.split(key_blocks, per_device)

    def one_block(key_block):
        key_order, key_local = jax.random.split(key_block, 2)
        picked = jax.random.permutation(key_order, chosen)
        local_row = jax.random.randint(key_local, (requests,), 0, ROWS_DEV, dtype=jnp.int32)
        return (picked * ROWS_DEV + local_row).reshape(TGT_DEV, NEIGH)
    return jax.vmap(one_block)(block_keys)


def draw_neighbor_ids(key, part):
    owners = NODES // ROWS_DEV
    keys_all = jax.random.split(jax.random.fold_in(key, 11), owners)
    return jax.vmap(draw_device)(keys_all).reshape(TARGETS, NEIGH)


def draw_bias(key, part):
    column_scale = 0.3 + 1.7 * jnp.arange(D, dtype=jnp.float32) / D
    values = jax.random.normal(jax.random.fold_in(key, 5), (D,), jnp.float32) * column_scale
    return jnp.clip(values, -6.0, 6.0)


def levels(own_key, shape, shards, smallest, top_value):
    gain = 1.0
    for axis_at, parts in shards:
        steps = jax.random.uniform(jax.random.fold_in(jax.random.fold_in(own_key, 6), axis_at), (parts,), jnp.float32, smallest / len(shards), top_value / len(shards))
        gain = gain * jnp.repeat(jnp.exp(steps), shape[axis_at] // parts).reshape((-1,) + (1,) * (len(shape) - 1 - axis_at))
    return gain


def centred(rng, extent, scale, limit, cuts=(), held_as=jnp.bfloat16):
    result = jax.random.normal(rng, extent, jnp.float32) * scale
    if len(cuts) > 0:
        result = levels(rng, extent, cuts, -0.22, 0.18) * result
    return jnp.clip(result, min=-limit, max=limit).astype(held_as)


def setup_inputs(seed: int = 0, part: int = 0) -> dict:
    keys = jax.random.split(jax.random.key(seed), 8)
    part_keys = jax.random.split(jax.random.fold_in(keys[7], part), 8)
    return {
        "feature_table": centred(part_keys[0], (NODES, D), 1.0, 6.0, ((0, 8), (1, 2)), jnp.float32),
        "own_features": centred(part_keys[1], (TARGETS, D), 1.0, 6.0, ((0, 8), (1, 2)), jnp.float32),
        "neighbor_ids": draw_neighbor_ids(jax.random.fold_in(jax.random.fold_in(keys[7], part), 71), part),
        "importance": jnp.clip(jnp.exp(math.log(5.0) - 2.3025851 * jax.random.uniform(part_keys[3], (TARGETS, NEIGH), jnp.float32) ** levels(part_keys[3], (TARGETS, NEIGH), ((0, 8),), -0.2, 0.2)), 0.5, 5.0),
        "w_self": centred(keys[4], (D, D), D ** -0.5, 0.1875, ((0, 2),)),
        "w_pool": centred(keys[5], (D, D), D ** -0.5, 0.1875, ((0, 2),)),
        "bias": draw_bias(jax.random.fold_in(keys[7], 71), part),
    }


def reference(feature_table, own_features, neighbor_ids, importance, w_self, w_pool, bias):
    weights = importance / lax.optimization_barrier(jnp.sum(importance, axis=1, keepdims=True))
    blocks = TARGETS // TGT_DEV

    def pool_block(operands):
        id_block, share_block = operands
        gathered = jnp.take(feature_table, id_block, axis=0)
        return lax.optimization_barrier(jnp.sum(share_block[:, :, None] * gathered, axis=1))
    pooled = lax.map(pool_block, (neighbor_ids.reshape(blocks, TGT_DEV, NEIGH), weights.reshape(blocks, TGT_DEV, NEIGH)))
    pooled = pooled.reshape(TARGETS, D)
    own_round = own_features.astype(jnp.bfloat16)
    pooled_round = pooled.astype(jnp.bfloat16)
    preact = jnp.dot(own_round, w_self, preferred_element_type=jnp.float32) + jnp.dot(pooled_round, w_pool, preferred_element_type=jnp.float32) + bias
    hidden = jnp.maximum(preact, 0.0)
    return hidden * lax.rsqrt(lax.optimization_barrier(jnp.mean(hidden * hidden, axis=1, keepdims=True)) + 1e-06)
```

```python
from functools import partial

import jax
import jax.numpy as jnp
from jax import lax
from jax.experimental import pallas as pl
from jax.experimental.pallas import tpu as pltpu
from jax.sharding import PartitionSpec as P

MESH = pl.DeviceIdType.MESH
LANES = 128
HALF = 64
SUB = 8


def kernel(
    n,
    peers_chunk,
    ids_ref,
    imp_ref,
    own_ref,
    bias_ref,
    table_hbm,
    ws_hbm,
    wp_hbm,
    out_ref,
    table_v,
    table_b,
    ws_v,
    wp_v,
    pack_send,
    packs,
    wmat,
    mine,
    psend,
    precv,
    fsend,
    frecv,
    local_sem,
    pack_ssem,
    pack_rsem,
    part_ssem,
    part_rsem,
    fin_sem,
):
    me = lax.axis_index("rows")
    col = lax.axis_index("cols")
    targets, neigh = ids_ref.shape
    rows_dev, width = table_v.shape
    groups = targets // SUB
    half_rows = targets // 2
    hi_count = rows_dev // LANES

    barrier = pltpu.get_barrier_semaphore()

    def greet(d, carry):
        pl.semaphore_signal(
            barrier, inc=1, device_id={"rows": lax.rem(me + d, n)}, device_id_type=MESH
        )
        return carry

    lax.fori_loop(1, n, greet, 0)
    pl.semaphore_signal(barrier, inc=1, device_id={"cols": 1 - col}, device_id_type=MESH)

    copies = (
        pltpu.make_async_copy(table_hbm, table_v, local_sem.at[0]),
        pltpu.make_async_copy(ws_hbm, ws_v, local_sem.at[1]),
        pltpu.make_async_copy(wp_hbm, wp_v, local_sem.at[2]),
    )
    for c in copies:
        c.start()

    pack_send[...] = jnp.full(pack_send.shape, -1.0, jnp.float32)
    for g in range(groups):
        for part in range(2):
            src = pl.ds(SUB * g + 4 * part, 4)
            dst = pl.ds(HALF * part, neigh)
            pack_send[pl.ds(4 * g, 4), dst] = ids_ref[src, :].astype(jnp.float32)
            pack_send[pl.ds(half_rows + 4 * g, 4), dst] = imp_ref[src, :]
    packs[0] = pack_send[...]

    pl.semaphore_wait(barrier, n)

    def pack_copy(d):
        return pltpu.make_async_remote_copy(
            src_ref=pack_send,
            dst_ref=packs.at[d],
            send_sem=pack_ssem.at[d],
            recv_sem=pack_rsem.at[d],
            device_id={"rows": lax.rem(me + d, n)},
            device_id_type=MESH,
        )

    def start_pack(d, carry):
        pack_copy(d).start()
        return carry

    lax.fori_loop(1, n, start_pack, 0)

    copies[0].wait()
    table_b[...] = table_v[...].astype(jnp.bfloat16)
    copies[1].wait()
    fsend[...] = jnp.dot(
        own_ref[...].astype(jnp.bfloat16), ws_v[...], preferred_element_type=jnp.float32
    )

    row_iota = lax.broadcasted_iota(jnp.int32, (LANES, LANES), 0).astype(jnp.float32)
    key_iota = lax.broadcasted_iota(jnp.int32, (hi_count * SUB, LANES), 0).astype(jnp.float32)
    lane = lax.broadcasted_iota(jnp.int32, (half_rows, LANES), 1)
    prow = lax.broadcasted_iota(jnp.int32, (half_rows, LANES), 0)
    t_of = (lax.rem(prow, 4) + jnp.where(lane >= HALF, 4, 0)).astype(jnp.float32)
    base = (me * rows_dev).astype(jnp.float32)

    def build(d, slot):
        ids = packs[d, pl.ds(0, half_rows), :]
        weight = packs[d, pl.ds(half_rows, half_rows), :]
        rel = ids - base
        valid = jnp.logical_and(rel >= 0.0, rel < float(rows_dev))
        high = jnp.floor(rel * (1.0 / LANES))
        low = rel - high * LANES
        key = jnp.where(valid, high * SUB + t_of, -1.0)
        for g in range(groups):
            lhs, rhs = [], []
            for c in range(4):
                r = 4 * g + c
                lhs.append(
                    jnp.where(key_iota == key[r : r + 1, :], weight[r : r + 1, :], 0.0).astype(
                        jnp.bfloat16
                    )
                )
                rhs.append(
                    jnp.where(row_iota == low[r : r + 1, :], 1.0, 0.0).astype(jnp.bfloat16)
                )
            block = lax.dot_general(
                jnp.concatenate(lhs, axis=1),
                jnp.concatenate(rhs, axis=1),
                (((1,), (1,)), ((), ())),
                preferred_element_type=jnp.float32,
            )
            row = pl.multiple_of(slot * targets + SUB * g, SUB)
            for h in range(hi_count):
                wmat[pl.ds(row, SUB), pl.ds(h * LANES, LANES)] = block[h * SUB : (h + 1) * SUB, :]

    def part_copy(d):
        return pltpu.make_async_remote_copy(
            src_ref=psend.at[d],
            dst_ref=precv.at[d],
            send_sem=part_ssem.at[d],
            recv_sem=part_rsem.at[d],
            device_id={"rows": lax.rem(me - d + n, n)},
            device_id_type=MESH,
        )

    def chunk(first, has_own):
        def one(s, carry):
            d = first + s
            pack_copy(d).wait_recv()
            build(d, s)
            return carry

        if has_own:
            build(0, 0)
        lax.fori_loop(1 if has_own else 0, peers_chunk, one, 0)
        sums = jnp.dot(
            wmat[...].astype(jnp.bfloat16), table_b[...], preferred_element_type=jnp.float32
        )
        for s in range(peers_chunk):
            rows = sums[s * targets : (s + 1) * targets, :]
            if has_own and s == 0:
                mine[...] = rows
            else:
                psend[first + s] = rows.astype(jnp.bfloat16)
                part_copy(first + s).start()

    chunk(0, True)

    def later(i, carry):
        chunk(i * peers_chunk, False)
        return carry

    lax.fori_loop(1, n // peers_chunk, later, 0)

    def collect(d, carry):
        part_copy(d).wait_recv()
        mine[...] += precv[d].astype(jnp.float32)
        return carry

    lax.fori_loop(1, n, collect, 0)
    pooled = mine[...] / jnp.sum(imp_ref[...], axis=1, keepdims=True)
    copies[2].wait()
    fsend[...] += jnp.dot(
        pooled.astype(jnp.bfloat16), wp_v[...], preferred_element_type=jnp.float32
    )
    swap = pltpu.make_async_remote_copy(
        src_ref=fsend,
        dst_ref=frecv,
        send_sem=fin_sem.at[0],
        recv_sem=fin_sem.at[1],
        device_id={"cols": 1 - col},
        device_id_type=MESH,
    )
    swap.start()
    swap.wait_recv()
    hidden = jnp.maximum(fsend[...] + frecv[...] + bias_ref[...], 0.0)
    scale = lax.rsqrt(jnp.mean(hidden * hidden, axis=1, keepdims=True) + 1e-06)
    half = jnp.where(col == 0, hidden[:, :width], hidden[:, width:])
    out_ref[...] = half * scale

    swap.wait_send()

    def drain(d, carry):
        pack_copy(d).wait_send()
        part_copy(d).wait_send()
        return carry

    lax.fori_loop(1, n, drain, 0)


def body(feature_table, own_features, neighbor_ids, importance, w_self, w_pool, bias):
    rows_dev, width = feature_table.shape
    targets, neigh = neighbor_ids.shape
    n = lax.axis_size("rows")
    full = w_self.shape[1]
    assert lax.axis_size("cols") == 2 and neigh <= HALF and targets % 16 == 0
    peers_chunk = 4 if n % 4 == 0 else 1
    vmem = pl.BlockSpec(memory_space=pltpu.VMEM)
    hbm = pl.BlockSpec(memory_space=pl.ANY)
    return pl.pallas_call(
        partial(kernel, n, peers_chunk),
        out_shape=jax.ShapeDtypeStruct((targets, width), jnp.float32),
        in_specs=[vmem, vmem, vmem, vmem, hbm, hbm, hbm],
        out_specs=vmem,
        scratch_shapes=[
            pltpu.VMEM((rows_dev, width), jnp.float32),
            pltpu.VMEM((rows_dev, width), jnp.bfloat16),
            pltpu.VMEM(w_self.shape, jnp.bfloat16),
            pltpu.VMEM(w_pool.shape, jnp.bfloat16),
            pltpu.VMEM((targets, LANES), jnp.float32),
            pltpu.VMEM((n, targets, LANES), jnp.float32),
            pltpu.VMEM((peers_chunk * targets, rows_dev), jnp.float32),
            pltpu.VMEM((targets, width), jnp.float32),
            pltpu.VMEM((n, targets, width), jnp.bfloat16),
            pltpu.VMEM((n, targets, width), jnp.bfloat16),
            pltpu.VMEM((targets, full), jnp.float32),
            pltpu.VMEM((targets, full), jnp.float32),
            pltpu.SemaphoreType.DMA((3,)),
            pltpu.SemaphoreType.DMA((n,)),
            pltpu.SemaphoreType.DMA((n,)),
            pltpu.SemaphoreType.DMA((n,)),
            pltpu.SemaphoreType.DMA((n,)),
            pltpu.SemaphoreType.DMA((2,)),
        ],
        compiler_params=pltpu.CompilerParams(collective_id=0, has_side_effects=True),
    )(
        neighbor_ids,
        importance,
        own_features,
        bias.reshape(1, full),
        feature_table,
        w_self,
        w_pool,
    )


def solution(mesh):
    placed = (
        P(("groups", "rows"), "cols"),
        P(("groups", "rows"), "cols"),
        P(("groups", "rows"), None),
        P(("groups", "rows"), None),
        P("cols", None),
        P("cols", None),
        P(),
    )
    return jax.shard_map(
        body, mesh=mesh, in_specs=placed, out_specs=P(("groups", "rows"), "cols"), check_vma=False
    )
```

```python
from functools import partial

import jax
import jax.numpy as jnp
from jax import lax
from jax.experimental import pallas as pl
from jax.experimental.pallas import tpu as pltpu
from jax.sharding import PartitionSpec as P

MESH = pl.DeviceIdType.MESH
LANES = 128
HALF = 64
SUB = 8
IMP_SCALE = 6000.0


def kernel(
    n,
    peers_chunk,
    ids_hbm,
    imp_hbm,
    own_hbm,
    bias_hbm,
    table_hbm,
    ws_hbm,
    wp_hbm,
    out_ref,
    ids_ref,
    imp_ref,
    own_ref,
    bias_ref,
    table_v,
    table_b,
    ws_v,
    wp_v,
    pack_in,
    pack_send,
    packs,
    wmat,
    mine,
    psend,
    precv,
    fsend,
    frecv,
    local_sem,
    pack_ssem,
    pack_rsem,
    part_ssem,
    part_rsem,
    fin_sem,
):
    me = lax.axis_index("rows")
    col = lax.axis_index("cols")
    targets, neigh = ids_ref.shape
    rows_dev, width = table_v.shape
    groups = targets // SUB
    half_rows = targets // 2
    hi_count = rows_dev // LANES

    barrier = pltpu.get_barrier_semaphore()

    def partner(k):
        peer, bit = me, 1
        while bit < n:
            peer = peer + lax.rem(k // bit, 2) * (1 - 2 * lax.rem(me // bit, 2)) * bit
            bit *= 2
        return peer

    def greet(d, carry):
        pl.semaphore_signal(
            barrier, inc=1, device_id={"rows": partner(d)}, device_id_type=MESH
        )
        return carry

    lax.fori_loop(1, n, greet, 0)
    pl.semaphore_signal(barrier, inc=1, device_id={"cols": 1 - col}, device_id_type=MESH)

    copies = tuple(
        pltpu.make_async_copy(src, dst, local_sem.at[i])
        for i, (src, dst) in enumerate(
            (
                (ids_hbm, ids_ref),
                (imp_hbm, imp_ref),
                (own_hbm, own_ref),
                (bias_hbm, bias_ref),
                (table_hbm, table_v),
                (ws_hbm, ws_v),
                (wp_hbm, wp_v),
            )
        )
    )
    for c in copies:
        c.start()
    copies[0].wait()
    copies[1].wait()

    pack_in[...] = jnp.full(pack_in.shape, -1, jnp.int32)
    for g in range(groups):
        for part in range(2):
            src = pl.ds(SUB * g + 4 * part, 4)
            dst = pl.ds(HALF * part, neigh)
            pack_in[pl.ds(4 * g, 4), dst] = ids_ref[src, :]
            pack_in[pl.ds(half_rows + 4 * g, 4), dst] = jnp.round(
                imp_ref[src, :] * IMP_SCALE
            ).astype(jnp.int32)

    def pack_for(k, carry):
        local = pack_in[pl.ds(0, half_rows), :] - partner(k) * rows_dev
        local = jnp.where(jnp.logical_and(local >= 0, local < rows_dev), local, -1)
        pack_send[k, pl.ds(0, half_rows), :] = local.astype(jnp.int16)
        pack_send[k, pl.ds(half_rows, half_rows), :] = pack_in[
            pl.ds(half_rows, half_rows), :
        ].astype(jnp.int16)
        return carry

    lax.fori_loop(0, n, pack_for, 0)
    packs[0] = pack_send[0]

    pl.semaphore_wait(barrier, n)

    def pack_copy(d):
        return pltpu.make_async_remote_copy(
            src_ref=pack_send.at[d],
            dst_ref=packs.at[d],
            send_sem=pack_ssem.at[d],
            recv_sem=pack_rsem.at[d],
            device_id={"rows": partner(d)},
            device_id_type=MESH,
        )

    def start_pack(i, carry):
        pack_copy(n - i).start()
        return carry

    lax.fori_loop(1, n, start_pack, 0)

    copies[4].wait()
    table_b[...] = table_v[...].astype(jnp.bfloat16)
    copies[2].wait()
    copies[5].wait()
    fsend[...] = jnp.dot(
        own_ref[...].astype(jnp.bfloat16), ws_v[...], preferred_element_type=jnp.float32
    )

    row_iota = lax.broadcasted_iota(jnp.int32, (LANES, LANES), 0).astype(jnp.float32)
    key_iota = lax.broadcasted_iota(jnp.int32, (hi_count * SUB, LANES), 0).astype(jnp.float32)
    lane = lax.broadcasted_iota(jnp.int32, (half_rows, LANES), 1)
    prow = lax.broadcasted_iota(jnp.int32, (half_rows, LANES), 0)
    t_of = (lax.rem(prow, 4) + jnp.where(lane >= HALF, 4, 0)).astype(jnp.float32)

    def build(d, slot):
        rel = packs[d, pl.ds(0, half_rows), :].astype(jnp.int32).astype(jnp.float32)
        weight = packs[d, pl.ds(half_rows, half_rows), :].astype(jnp.int32).astype(jnp.float32)
        high = jnp.floor(rel * (1.0 / LANES))
        low = rel - high * LANES
        key = jnp.where(rel >= 0.0, high * SUB + t_of, -1.0)
        for g in range(groups):
            lhs, rhs = [], []
            for c in range(4):
                r = 4 * g + c
                lhs.append(
                    jnp.where(key_iota == key[r : r + 1, :], weight[r : r + 1, :], 0.0).astype(
                        jnp.bfloat16
                    )
                )
                rhs.append(
                    jnp.where(row_iota == low[r : r + 1, :], 1.0, 0.0).astype(jnp.bfloat16)
                )
            block = lax.dot_general(
                jnp.concatenate(lhs, axis=1),
                jnp.concatenate(rhs, axis=1),
                (((1,), (1,)), ((), ())),
                preferred_element_type=jnp.float32,
            )
            row = pl.multiple_of(slot * targets + SUB * g, SUB)
            for h in range(hi_count):
                wmat[pl.ds(row, SUB), pl.ds(h * LANES, LANES)] = block[h * SUB : (h + 1) * SUB, :]

    def part_copy(d):
        return pltpu.make_async_remote_copy(
            src_ref=psend.at[d],
            dst_ref=precv.at[d],
            send_sem=part_ssem.at[d],
            recv_sem=part_rsem.at[d],
            device_id={"rows": partner(d)},
            device_id_type=MESH,
        )

    def chunk(first, has_own):
        def one(s, carry):
            d = first - s
            pack_copy(d).wait_recv()
            build(d, s)
            return carry

        lax.fori_loop(0, peers_chunk - 1 if has_own else peers_chunk, one, 0)
        if has_own:
            build(0, peers_chunk - 1)
        sums = jnp.dot(
            wmat[...].astype(jnp.bfloat16), table_b[...], preferred_element_type=jnp.float32
        )
        for s in range(peers_chunk):
            rows = sums[s * targets : (s + 1) * targets, :]
            if has_own and s == peers_chunk - 1:
                mine[...] = rows
            else:
                psend[first - s] = rows.astype(jnp.bfloat16)
                part_copy(first - s).start()

    def later(i, carry):
        chunk(n - 1 - i * peers_chunk, False)
        return carry

    lax.fori_loop(0, n // peers_chunk - 1, later, 0)
    chunk(peers_chunk - 1, True)

    def collect(i, carry):
        d = n - i
        part_copy(d).wait_recv()
        mine[...] += precv[d].astype(jnp.float32)
        return carry

    lax.fori_loop(1, n, collect, 0)
    pooled = mine[...] / (IMP_SCALE * jnp.sum(imp_ref[...], axis=1, keepdims=True))
    copies[6].wait()
    fsend[...] += jnp.dot(
        pooled.astype(jnp.bfloat16), wp_v[...], preferred_element_type=jnp.float32
    )
    swap = pltpu.make_async_remote_copy(
        src_ref=fsend,
        dst_ref=frecv,
        send_sem=fin_sem.at[0],
        recv_sem=fin_sem.at[1],
        device_id={"cols": 1 - col},
        device_id_type=MESH,
    )
    swap.start()
    copies[3].wait()
    swap.wait_recv()
    hidden = jnp.maximum(fsend[...] + frecv[...] + bias_ref[...], 0.0)
    scale = lax.rsqrt(jnp.mean(hidden * hidden, axis=1, keepdims=True) + 1e-06)
    half = jnp.where(col == 0, hidden[:, :width], hidden[:, width:])
    out_ref[...] = half * scale

    swap.wait_send()

    def drain(d, carry):
        pack_copy(d).wait_send()
        part_copy(d).wait_send()
        return carry

    lax.fori_loop(1, n, drain, 0)


def body(feature_table, own_features, neighbor_ids, importance, w_self, w_pool, bias):
    rows_dev, width = feature_table.shape
    targets, neigh = neighbor_ids.shape
    n = lax.axis_size("rows")
    full = w_self.shape[1]
    assert lax.axis_size("cols") == 2 and neigh <= HALF and targets % 16 == 0
    assert n & (n - 1) == 0 and n > 1
    peers_chunk = 2
    vmem = pl.BlockSpec(memory_space=pltpu.VMEM)
    hbm = pl.BlockSpec(memory_space=pl.ANY)
    return pl.pallas_call(
        partial(kernel, n, peers_chunk),
        out_shape=pltpu.VMEM((targets, width), jnp.float32),
        in_specs=[hbm] * 7,
        out_specs=vmem,
        scratch_shapes=[
            pltpu.VMEM((targets, neigh), jnp.int32),
            pltpu.VMEM((targets, neigh), jnp.float32),
            pltpu.VMEM((targets, width), jnp.float32),
            pltpu.VMEM((1, full), jnp.float32),
            pltpu.VMEM((rows_dev, width), jnp.float32),
            pltpu.VMEM((rows_dev, width), jnp.bfloat16),
            pltpu.VMEM(w_self.shape, jnp.bfloat16),
            pltpu.VMEM(w_pool.shape, jnp.bfloat16),
            pltpu.VMEM((targets, LANES), jnp.int32),
            pltpu.VMEM((n, targets, LANES), jnp.int16),
            pltpu.VMEM((n, targets, LANES), jnp.int16),
            pltpu.VMEM((peers_chunk * targets, rows_dev), jnp.float32),
            pltpu.VMEM((targets, width), jnp.float32),
            pltpu.VMEM((n, targets, width), jnp.bfloat16),
            pltpu.VMEM((n, targets, width), jnp.bfloat16),
            pltpu.VMEM((targets, full), jnp.float32),
            pltpu.VMEM((targets, full), jnp.float32),
            pltpu.SemaphoreType.DMA((7,)),
            pltpu.SemaphoreType.DMA((n,)),
            pltpu.SemaphoreType.DMA((n,)),
            pltpu.SemaphoreType.DMA((n,)),
            pltpu.SemaphoreType.DMA((n,)),
            pltpu.SemaphoreType.DMA((2,)),
        ],
        compiler_params=pltpu.CompilerParams(collective_id=0, has_side_effects=True),
    )(
        neighbor_ids,
        importance,
        own_features,
        bias.reshape(1, full),
        feature_table,
        w_self,
        w_pool,
    )


def solution(mesh):
    placed = (
        P(("groups", "rows"), "cols"),
        P(("groups", "rows"), "cols"),
        P(("groups", "rows"), None),
        P(("groups", "rows"), None),
        P("cols", None),
        P("cols", None),
        P(),
    )
    return jax.shard_map(
        body, mesh=mesh, in_specs=placed, out_specs=P(("groups", "rows"), "cols"), check_vma=False
    )
```

```python
from functools import partial

import jax
import jax.numpy as jnp
from jax import lax
from jax.experimental import pallas as pl
from jax.experimental.pallas import tpu as pltpu
from jax.sharding import PartitionSpec as P

MESH = pl.DeviceIdType.MESH
LANES = 128
HALF = 64
SUB = 8
IMP_SCALE = 6000.0


def kernel(
    n,
    peers_chunk,
    ids_hbm,
    imp_hbm,
    own_hbm,
    bias_hbm,
    table_hbm,
    ws_hbm,
    wp_hbm,
    out_ref,
    ids_ref,
    imp_ref,
    own_ref,
    bias_ref,
    table_v,
    table_b,
    ws_v,
    wp_v,
    pack_in,
    pack_send,
    packs,
    wmat,
    mine,
    psend,
    precv,
    fsend,
    frecv,
    local_sem,
    pack_ssem,
    pack_rsem,
    part_ssem,
    part_rsem,
    fin_ssem,
    fin_rsem,
):
    me = lax.axis_index("rows")
    col = lax.axis_index("cols")
    targets, neigh = ids_ref.shape
    rows_dev, width = table_v.shape
    groups = targets // SUB
    half_rows = targets // 2
    hi_count = rows_dev // LANES

    barrier = pltpu.get_barrier_semaphore()

    flips, bit = [], 1
    while bit < n:
        flips.append((bit, (1 - 2 * lax.rem(lax.div(me, bit), 2)) * bit))
        bit *= 2

    def partner(k):
        peer = me
        for bit, flip in flips:
            if isinstance(k, int):
                peer = peer + flip if k // bit % 2 else peer
            else:
                peer = peer + lax.rem(lax.div(k, bit), 2) * flip
        return peer

    def each(first, last, step):
        if n <= 16:
            for i in range(first, last):
                step(i)
        else:

            def body(i, carry):
                step(i)
                return carry

            lax.fori_loop(first, last, body, 0)

    def greet(i):
        pl.semaphore_signal(
            barrier, inc=1, device_id={"rows": partner(n - i)}, device_id_type=MESH
        )

    copies = tuple(
        pltpu.make_async_copy(src, dst, local_sem.at[i])
        for i, (src, dst) in enumerate(
            (
                (ids_hbm, ids_ref),
                (imp_hbm, imp_ref),
                (own_hbm, own_ref),
                (bias_hbm, bias_ref),
                (table_hbm, table_v),
                (ws_hbm, ws_v),
                (wp_hbm, wp_v),
            )
        )
    )
    copies[0].start()
    copies[1].start()
    each(1, n, greet)
    pl.semaphore_signal(barrier, inc=1, device_id={"cols": 1 - col}, device_id_type=MESH)
    for c in copies[2:]:
        c.start()
    copies[0].wait()
    copies[1].wait()

    pack_in[...] = jnp.full(pack_in.shape, -1, jnp.int32)
    for g in range(groups):
        for part in range(2):
            src = pl.ds(SUB * g + 4 * part, 4)
            dst = pl.ds(HALF * part, neigh)
            pack_in[pl.ds(4 * g, 4), dst] = ids_ref[src, :]
            pack_in[pl.ds(half_rows + 4 * g, 4), dst] = jnp.round(
                imp_ref[src, :] * IMP_SCALE
            ).astype(jnp.int32)

    def pack_for(k):
        local = pack_in[pl.ds(0, half_rows), :] - partner(k) * rows_dev
        local = jnp.where(jnp.logical_and(local >= 0, local < rows_dev), local, -1)
        pack_send[k, pl.ds(0, half_rows), :] = local.astype(jnp.int16)
        pack_send[k, pl.ds(half_rows, half_rows), :] = pack_in[
            pl.ds(half_rows, half_rows), :
        ].astype(jnp.int16)

    each(0, n, pack_for)
    packs[0] = pack_send[0]

    pl.semaphore_wait(barrier, n)

    def pack_copy(d):
        return pltpu.make_async_remote_copy(
            src_ref=pack_send.at[d],
            dst_ref=packs.at[d],
            send_sem=pack_ssem.at[d],
            recv_sem=pack_rsem.at[d],
            device_id={"rows": partner(d)},
            device_id_type=MESH,
        )

    each(1, n, lambda i: pack_copy(n - i).start())

    copies[4].wait()
    table_b[...] = table_v[...].astype(jnp.bfloat16)
    copies[2].wait()
    copies[5].wait()
    own = own_ref[...].astype(jnp.bfloat16)
    for h in range(2):
        fsend[h] = jnp.dot(
            own, ws_v[:, h * width : (h + 1) * width], preferred_element_type=jnp.float32
        )

    row_iota = lax.broadcasted_iota(jnp.int32, (LANES, LANES), 0).astype(jnp.float32)
    key_iota = lax.broadcasted_iota(jnp.int32, (hi_count * SUB, LANES), 0).astype(jnp.float32)
    lane = lax.broadcasted_iota(jnp.int32, (half_rows, LANES), 1)
    prow = lax.broadcasted_iota(jnp.int32, (half_rows, LANES), 0)
    t_of = (lax.rem(prow, 4) + jnp.where(lane >= HALF, 4, 0)).astype(jnp.float32)

    def build(d, slot):
        rel = packs[d, pl.ds(0, half_rows), :].astype(jnp.int32).astype(jnp.float32)
        weight = packs[d, pl.ds(half_rows, half_rows), :].astype(jnp.int32).astype(jnp.float32)
        high = jnp.floor(rel * (1.0 / LANES))
        low = rel - high * LANES
        key = jnp.where(rel >= 0.0, high * SUB + t_of, -1.0)
        for g in range(groups):
            lhs, rhs = [], []
            for c in range(4):
                r = 4 * g + c
                lhs.append(
                    jnp.where(key_iota == key[r : r + 1, :], weight[r : r + 1, :], 0.0).astype(
                        jnp.bfloat16
                    )
                )
                rhs.append(
                    jnp.where(row_iota == low[r : r + 1, :], 1.0, 0.0).astype(jnp.bfloat16)
                )
            block = lax.dot_general(
                jnp.concatenate(lhs, axis=1),
                jnp.concatenate(rhs, axis=1),
                (((1,), (1,)), ((), ())),
                preferred_element_type=jnp.float32,
            )
            row = pl.multiple_of(slot * targets + SUB * g, SUB)
            for h in range(hi_count):
                wmat[pl.ds(row, SUB), pl.ds(h * LANES, LANES)] = block[h * SUB : (h + 1) * SUB, :]

    def part_copy(d):
        return pltpu.make_async_remote_copy(
            src_ref=psend.at[d],
            dst_ref=precv.at[d],
            send_sem=part_ssem.at[d],
            recv_sem=part_rsem.at[d],
            device_id={"rows": partner(d)},
            device_id_type=MESH,
        )

    def chunk(first, has_own):
        def one(s, carry):
            d = first - s
            pack_copy(d).wait_recv()
            build(d, s)
            return carry

        if has_own:
            build(0, peers_chunk - 1)
        lax.fori_loop(0, peers_chunk - 1 if has_own else peers_chunk, one, 0)
        sums = jnp.dot(
            wmat[...].astype(jnp.bfloat16), table_b[...], preferred_element_type=jnp.float32
        )
        for s in range(peers_chunk):
            rows = sums[s * targets : (s + 1) * targets, :]
            if has_own and s == peers_chunk - 1:
                mine[...] = rows
            else:
                psend[first - s] = rows.astype(jnp.bfloat16)
                part_copy(first - s).start()

    chunk(peers_chunk - 1, True)
    each(0, n // peers_chunk - 1, lambda i: chunk(n - 1 - i * peers_chunk, False))
    inverse = 1.0 / (IMP_SCALE * jnp.sum(imp_ref[...], axis=1, keepdims=True))
    copies[6].wait()
    copies[3].wait()

    def collect(i):
        d = n - i
        part_copy(d).wait_recv()
        mine[...] += precv[d].astype(jnp.float32)

    each(1, n, collect)
    pooled = (mine[...] * inverse).astype(jnp.bfloat16)

    def swap(h):
        return pltpu.make_async_remote_copy(
            src_ref=fsend.at[h],
            dst_ref=frecv.at[h],
            send_sem=fin_ssem.at[h],
            recv_sem=fin_rsem.at[h],
            device_id={"cols": 1 - col},
            device_id_type=MESH,
        )

    for h in range(2):
        fsend[h] += jnp.dot(
            pooled, wp_v[:, h * width : (h + 1) * width], preferred_element_type=jnp.float32
        )
        swap(h).start()
    hidden = []
    for h in range(2):
        swap(h).wait_recv()
        hidden.append(
            jnp.maximum(fsend[h] + frecv[h] + bias_ref[:, h * width : (h + 1) * width], 0.0)
        )
    square = jnp.sum(hidden[0] * hidden[0] + hidden[1] * hidden[1], axis=1, keepdims=True)
    scale = lax.rsqrt(square * (0.5 / width) + 1e-06)
    out_ref[...] = jnp.where(col == 0, hidden[0], hidden[1]) * scale

    swap(0).wait_send()
    swap(1).wait_send()

    def drain(d):
        pack_copy(d).wait_send()
        part_copy(d).wait_send()

    each(1, n, drain)


def body(feature_table, own_features, neighbor_ids, importance, w_self, w_pool, bias):
    rows_dev, width = feature_table.shape
    targets, neigh = neighbor_ids.shape
    n = lax.axis_size("rows")
    full = w_self.shape[1]
    assert lax.axis_size("cols") == 2 and full == 2 * width and neigh <= HALF and targets % 16 == 0
    assert n & (n - 1) == 0 and n > 1
    peers_chunk = 2
    vmem = pl.BlockSpec(memory_space=pltpu.VMEM)
    hbm = pl.BlockSpec(memory_space=pl.ANY)
    return pl.pallas_call(
        partial(kernel, n, peers_chunk),
        out_shape=pltpu.VMEM((targets, width), jnp.float32),
        in_specs=[hbm] * 7,
        out_specs=vmem,
        scratch_shapes=[
            pltpu.VMEM((targets, neigh), jnp.int32),
            pltpu.VMEM((targets, neigh), jnp.float32),
            pltpu.VMEM((targets, width), jnp.float32),
            pltpu.VMEM((1, full), jnp.float32),
            pltpu.VMEM((rows_dev, width), jnp.float32),
            pltpu.VMEM((rows_dev, width), jnp.bfloat16),
            pltpu.VMEM(w_self.shape, jnp.bfloat16),
            pltpu.VMEM(w_pool.shape, jnp.bfloat16),
            pltpu.VMEM((targets, LANES), jnp.int32),
            pltpu.VMEM((n, targets, LANES), jnp.int16),
            pltpu.VMEM((n, targets, LANES), jnp.int16),
            pltpu.VMEM((peers_chunk * targets, rows_dev), jnp.float32),
            pltpu.VMEM((targets, width), jnp.float32),
            pltpu.VMEM((n, targets, width), jnp.bfloat16),
            pltpu.VMEM((n, targets, width), jnp.bfloat16),
            pltpu.VMEM((2, targets, width), jnp.float32),
            pltpu.VMEM((2, targets, width), jnp.float32),
            pltpu.SemaphoreType.DMA((7,)),
            pltpu.SemaphoreType.DMA((n,)),
            pltpu.SemaphoreType.DMA((n,)),
            pltpu.SemaphoreType.DMA((n,)),
            pltpu.SemaphoreType.DMA((n,)),
            pltpu.SemaphoreType.DMA((2,)),
            pltpu.SemaphoreType.DMA((2,)),
        ],
        compiler_params=pltpu.CompilerParams(collective_id=0, has_side_effects=True),
    )(
        neighbor_ids,
        importance,
        own_features,
        bias.reshape(1, full),
        feature_table,
        w_self,
        w_pool,
    )


def solution(mesh):
    placed = (
        P(("groups", "rows"), "cols"),
        P(("groups", "rows"), "cols"),
        P(("groups", "rows"), None),
        P(("groups", "rows"), None),
        P("cols", None),
        P("cols", None),
        P(),
    )
    return jax.shard_map(
        body, mesh=mesh, in_specs=placed, out_specs=P(("groups", "rows"), "cols"), check_vma=False
    )
```
